1024 devices in a mesh: gx: 4 (over y_hi, core), gy: 16 (over z), gz: 16 (over y_lo, x).
Axes of the slice: x: 4, y: 8 (y_hi: 2, y_lo: 4; y = y_hi * 4 + y_lo), z: 16, core: 2. Of those that a mesh axis runs over, the one named last changes fastest.
Arguments:
- source: float32 [32, 256, 2048], P('gx', 'gy', 'gz'), may hold values from -18 to 18
- pressure_old: float32 [32, 256, 2048], P('gx', 'gy', 'gz'), may hold values from -6 to 6
- strain_prev: float32 [32, 256, 2048], P('gx', 'gy', 'gz'), may hold values from -6 to 6
- motion_old: float32 [3, 32, 256, 2048], P(None, 'gx', 'gy', 'gz'), may hold values from -6 to 6
- body_force: float32 [3, 32, 256, 2048], P(None, 'gx', 'gy', 'gz'), may hold values from -6 to 6
- zone_ids: int32 [32, 256, 2048], P('gx', 'gy', 'gz'), may hold values from 0 to 7
- drained: int32 [32, 256, 2048], P('gx', 'gy', 'gz'), may hold values 0 or 1
- perm_table: float32 [8], replicated, may hold values from 0.1 to 3
- lame_table: float32 [8], replicated, may hold values from 0.5 to 4
- shear_table: float32 [8], replicated, may hold values from 0.3 to 2
Outputs:
- pressure: float32 [32, 256, 2048], P('gx', 'gy', 'gz')
- motion: float32 [3, 32, 256, 2048], P(None, 'gx', 'gy', 'gz')
- strain: float32 [32, 256, 2048], P('gx', 'gy', 'gz')
The draws below stay inside these ranges and needn't reach their ends.
All inputs are finite; a program needn't handle non-finite values. No bound on the sum of `drained` on one device may be relied on, other than what follows from the above.
Results may differ from the reference program's by a relative error of at most 0.0001.
Values sent between devices are 32-bit elements; how exact they have to be, the bound alone decides.
A program may use at most 32 MiB of HBM per device.

```python
import math
import jax
import jax.numpy as jnp

ITERS = 2
ZONES = 8
NX = 32
NY = 256
NZ = 2048


def draw_source(key, part):
    rising = jnp.arange(NX, dtype=jnp.float32) / max(NX - 1, 1)
    base = jnp.clip(jax.random.normal(key, (NX, NY, NZ), jnp.float32), -6.0, 6.0)
    return base * (1.0 + 2.0 * rising)[:, None, None]


def place_ends(values, key, least, high):
    index_at = [jax.random.randint(jax.random.fold_in(key, axis), (), 0, length) for axis, length in enumerate(values.shape)]
    widest = values.shape.index(max(values.shape))
    neighbour = index_at[:widest] + [(index_at[widest] + 1) % values.shape[widest]] + index_at[widest + 1:]
    return values.at[tuple(index_at)].set(least).at[tuple(neighbour)].set(high)


def levels(rng, dims, pieces, low, high):
    factor_of, own = 1.0, jax.random.fold_in(rng, 6)
    for dim, blocks in pieces:
        draws = jnp.exp(jax.random.uniform(jax.random.fold_in(own, dim), (blocks,), jnp.float32, low / len(pieces), high / len(pieces)))
        factor_of = factor_of * jnp.repeat(draws, dims[dim] // blocks).reshape([-1 if axis == dim else 1 for axis in range(len(dims))])
    return factor_of


def scatter_about(own_key, extent, width, reach, shards=(), kind=jnp.bfloat16):
    level = levels(own_key, extent, shards, -0.22, 0.18) if shards else 1.0
    array = jax.random.normal(own_key, extent, jnp.float32) * width * level
    return jnp.minimum(jnp.maximum(array, -reach), reach).astype(kind)


def setup_inputs(seed: int = 0) -> dict:
    key_list = jax.random.split(jax.random.key(seed), 11)
    return {
        "source": draw_source(jax.random.fold_in(key_list[10], 71), 0),
        "pressure_old": scatter_about(key_list[1], (NX, NY, NZ), 1.0, 6.0, ((0, 4), (1, 16), (2, 16)), jnp.float32),
        "strain_prev": scatter_about(key_list[2], (NX, NY, NZ), 0.5, 6.0, ((0, 4), (1, 16), (2, 16)), jnp.float32),
        "motion_old": scatter_about(key_list[3], (3, NX, NY, NZ), 0.5, 6.0, ((1, 4), (2, 16), (3, 16)), jnp.float32),
        "body_force": scatter_about(key_list[4], (3, NX, NY, NZ), 1.0, 6.0, ((1, 4), (2, 16), (3, 16)), jnp.float32),
        "zone_ids": place_ends(jax.random.randint(key_list[5], (NX, NY, NZ), 0, ZONES), jax.random.fold_in(key_list[5], 1), 0, ZONES - 1).astype(jnp.int32),
        "drained": place_ends((jax.random.randint(key_list[6], (NX, NY, NZ), 0, 4) < 1).astype(jnp.int32), jax.random.fold_in(key_list[6], 1), 0, 1),
        "perm_table": jnp.clip(jnp.exp(jax.random.uniform(key_list[7], (ZONES,), jnp.float32, math.log(0.1), math.log(3.0))), 0.1, 3.0),
        "lame_table": jnp.clip(jnp.exp(jax.random.uniform(key_list[8], (ZONES,), jnp.float32, math.log(0.5), math.log(4.0))), 0.5, 4.0),
        "shear_table": jnp.clip(jnp.exp(jax.random.uniform(key_list[9], (ZONES,), jnp.float32, math.log(0.3), math.log(2.0))), 0.3, 2.0),
    }


storage = 0.2
biot_coef = 0.8
time_step = 1.0
leakage = 2.0
support = 1.0

def lookup(zone_ids, lookup_table):
    result = jnp.zeros(zone_ids.shape, jnp.float32)
    for zone_index in range(ZONES):
        result = result + jnp.where(zone_ids == zone_index, lookup_table[zone_index], 0.0)
    return result

def interior(padded):
    return padded[..., 1:-1, 1:-1, 1:-1]

def neighbours(padded):
    return [padded[..., 2:, 1:-1, 1:-1], padded[..., :-2, 1:-1, 1:-1], padded[..., 1:-1, 2:, 1:-1], padded[..., 1:-1, :-2, 1:-1], padded[..., 1:-1, 1:-1, 2:], padded[..., 1:-1, 1:-1, :-2]]

def harmonic(own_value, beside):
    return 2.0 * own_value * beside / (own_value + beside)

def central_div(motion_pad):
    return 0.5 * (motion_pad[0, 2:, 1:-1, 1:-1] - motion_pad[0, :-2, 1:-1, 1:-1] + (motion_pad[1, 1:-1, 2:, 1:-1] - motion_pad[1, 1:-1, :-2, 1:-1]) + (motion_pad[2, 1:-1, 1:-1, 2:] - motion_pad[2, 1:-1, 1:-1, :-2]))

def central_grad(press_pad):
    sided = neighbours(press_pad)
    return jnp.stack([0.5 * (sided[0] - sided[1]), 0.5 * (sided[2] - sided[3]), 0.5 * (sided[4] - sided[5])])

def conjugate(start_pad, rhs, diag, apply_padded, faces):
    iterate = interior(start_pad)
    residual = rhs - apply_padded(start_pad)
    precond = residual / diag
    image = apply_padded(faces(precond))
    gamma_now = jnp.sum(residual * precond)
    curvature = jnp.sum(precond * image)
    step_len = gamma_now / curvature
    direction = precond
    along = image
    for iteration in range(ITERS):
        iterate = iterate + step_len * direction
        residual = residual - step_len * along
        if iteration + 1 < ITERS:
            precond = residual / diag
            image = apply_padded(faces(precond))
            gamma_new = jnp.sum(residual * precond)
            curvature = jnp.sum(precond * image)
            momentum = gamma_new / gamma_now
            step_len = gamma_new / (curvature - momentum * gamma_new / step_len)
            direction = precond + momentum * direction
            along = image + momentum * along
            gamma_now = gamma_new
    return iterate

def pad_scalar(values):
    return jnp.pad(values, 1)

def pad_vector(values):
    return jnp.pad(values, ((0, 0), (1, 1), (1, 1), (1, 1)))

def reference(source, pressure_old, strain_prev, motion_old, body_force, zone_ids, drained, perm_table, lame_table, shear_table):
    permeability = lookup(zone_ids, perm_table)
    lame_first = lookup(zone_ids, lame_table)
    shear_mod = lookup(zone_ids, shear_table)
    fixed_term = biot_coef * biot_coef / (lame_first + 2.0 * shear_mod / 3.0)
    perm_pad = pad_scalar(permeability)
    heft_pad = pad_scalar(lame_first + shear_mod)
    shear_pad = pad_scalar(shear_mod)
    press_pad = pad_scalar(pressure_old)
    motion_pad = pad_vector(motion_old)
    transmit = [harmonic(permeability, beside) for beside in neighbours(perm_pad)]
    reaction = storage + fixed_term + leakage * drained.astype(jnp.float32)
    pdiag = reaction + time_step * sum(transmit)

    def apply_pressure(padded):
        center = interior(padded)
        flux = sum((factor * (center - beside) for factor, beside in zip(transmit, neighbours(padded))))
        return reaction * center + time_step * flux
    prhs = source + (storage + fixed_term) * pressure_old - biot_coef * (central_div(motion_pad) - strain_prev)
    pressure = conjugate(press_pad, prhs, pdiag, apply_pressure, pad_scalar)
    heft = interior(heft_pad)
    shear_faces = [harmonic(shear_mod, beside) for beside in neighbours(shear_pad)]
    heft_sides = neighbours(heft_pad)
    base_diag = support + sum(shear_faces) + heft
    ediag = jnp.stack([base_diag + heft_sides[1], base_diag + heft_sides[3], base_diag + heft_sides[5]])

    def apply_motion(padded):
        center = interior(padded)
        spread = sum((factor * (center - beside) for factor, beside in zip(shear_faces, neighbours(padded))))
        diverg = padded[0, 1:, :-1, :-1] - padded[0, :-1, :-1, :-1] + (padded[1, :-1, 1:, :-1] - padded[1, :-1, :-1, :-1]) + (padded[2, :-1, :-1, 1:] - padded[2, :-1, :-1, :-1])
        scaled = heft_pad[:-1, :-1, :-1] * diverg
        own_part = scaled[1:, 1:, 1:]
        push = jnp.stack([scaled[:-1, 1:, 1:] - own_part, scaled[1:, :-1, 1:] - own_part, scaled[1:, 1:, :-1] - own_part])
        return support * center + spread + push
    erhs = body_force - biot_coef * central_grad(pad_scalar(pressure))
    motion = conjugate(motion_pad, erhs, ediag, apply_motion, pad_vector)
    strain = central_div(pad_vector(motion))
    return (pressure, motion, strain)
```

```python
import functools

import jax
import jax.numpy as jnp
from jax import lax
from jax.experimental import pallas as pl
from jax.experimental.pallas import tpu as pltpu
from jax.sharding import PartitionSpec as P

ZONES = 8
MESH = pl.DeviceIdType.MESH
F32 = jnp.float32
WIN = (4, 24)
OWN = (8, 16)
L, R = (16, 17)


def lanes(rows):
    return lax.broadcasted_iota(jnp.int32, (rows, 128), 1)


class Row:
    def __init__(self, i, window, strip):
        self.i, self.strip = (i, strip)
        self.start, self.count = window
        self.lane = lanes(self.count)

    def at(self, ref, f, dy=0, i=None):
        return ref[f, self.i if i is None else i, pl.ds(self.start + dy, self.count), :]

    def xp(self, ref, f):
        if self.strip:
            return pltpu.roll(self.at(ref, f), 120, 1)
        return self.at(ref, f, i=self.i + 1)

    def xm(self, ref, f):
        if self.strip:
            return pltpu.roll(self.at(ref, f), 8, 1)
        return self.at(ref, f, i=self.i - 1)

    def yp(self, ref, f):
        return self.at(ref, f, dy=1)

    def ym(self, ref, f):
        return self.at(ref, f, dy=-1)

    def zp(self, ref, f):
        turned = pltpu.roll(self.at(ref, f), 127, 1)
        if self.strip:
            return turned
        edge = pltpu.roll(self.at(ref, f, i=R), 123 - 8 * self.i, 1)
        return jnp.where(self.lane == 127, edge, turned)

    def zm(self, ref, f):
        turned = pltpu.roll(self.at(ref, f), 1, 1)
        if self.strip:
            return turned
        edge = pltpu.roll(self.at(ref, f, i=L), 125 - 8 * self.i, 1)
        return jnp.where(self.lane == 0, edge, turned)

    def put(self, ref, f, value):
        ref[f, self.i, pl.ds(self.start, self.count), :] = value


def over_rows(low, high, body, window=WIN, strips=(L, R)):
    @pl.loop(low, high)
    def _(i):
        body(Row(i, window, False))

    if strips:

        @pl.loop(strips[0], strips[-1] + 1)
        def _(i):
            body(Row(i, window, True))


def harmonic(own, beside):
    total = own + beside
    return 2.0 * own * beside / jnp.where(total > 0.0, total, 1.0)


def fold(value):
    return value[0:8] + value[8:16]


def kernel(
    sizes,
    source,
    press_old,
    strain_prev,
    motion_old,
    body_force,
    zones,
    drained,
    perm_t,
    lame_t,
    shear_t,
    press_out,
    motion_out,
    strain_out,
    own_src,
    own_strain,
    own_bf,
    own_zone,
    own_drain,
    zd,
    xu,
    z0,
    ze,
    mat,
    tf,
    mf,
    diag,
    ediag,
    sp,
    gv,
    se,
    mo,
    pk_zd,
    pk_xu,
    pk_z0,
    pk_ze,
    pl_zd,
    pl_xu,
    pl_z0,
    pl_ze,
    pr_zd,
    pr_xu,
    pr_z0,
    pr_ze,
    ys_zd,
    ys_xu,
    ys_z0,
    ys_ze,
    yr_zd,
    yr_xu,
    yr_z0,
    yr_ze,
    rows,
    part,
    got_a,
    got_b,
    got_c,
    load_sem,
    xs_sem,
    xr_sem,
    zs_sem,
    zr_sem,
    yss_sem,
    yrs_sem,
    rs_sem,
    rr_sem,
    known,
):
    nx, ny, nz, cores, xs = sizes
    gx, gy, gz = (lax.axis_index("gx"), lax.axis_index("gy"), lax.axis_index("gz"))
    yhs, yls = (nx // cores, nz // xs)
    x_lo, x_hi = (gx > 0, gx < nx - 1)
    y_lo, y_hi = (gy > 0, gy < ny - 1)
    z_lo, z_hi = (gz > 0, gz < nz - 1)

    def turn(value, by, count):
        return lax.rem(value + (by % count), count)

    beside = []
    for by in (1, -1):
        if nx > 1:
            beside.append((turn(gx, by, nx), gy, gz))
        if ny > 1:
            beside.append((gx, turn(gy, by, ny), gz))
        if nz > 1:
            beside.append((gx, gy, turn(gz, by, nz)))
    yh, core = (gx // cores, lax.rem(gx, cores))
    yl, xx = (gz // xs, lax.rem(gz, xs))
    group_a = [
        (yh * cores + turn(core, c, cores), gy, yl * xs + turn(xx, x, xs))
        for c in range(cores)
        for x in range(xs)
        if c or x
    ]
    group_b = [
        (turn(yh, h, yhs) * cores + core, gy, turn(yl, k, yls) * xs + xx)
        for h in range(yhs)
        for k in range(yls)
        if h or k
    ]
    group_c = [(gx, turn(gy, k, ny), gz) for k in range(1, ny)]
    reach = 4
    if ny > 2 * reach + 1:
        near = [(gx, turn(gy, s * k, ny), gz) for k in range(1, reach + 1) for s in (1, -1)]
    else:
        near = group_c
    greet = beside + group_a + group_b + near

    barrier = pltpu.get_barrier_semaphore()
    for device in greet:
        pl.semaphore_signal(barrier, inc=1, device_id=device, device_id_type=MESH)

    loads = [
        pltpu.make_async_copy(zones, own_zone, load_sem.at[0]),
        pltpu.make_async_copy(drained, own_drain, load_sem.at[1]),
        pltpu.make_async_copy(press_old, xu.at[0, 4:12, 8:24, :], load_sem.at[2]),
        pltpu.make_async_copy(motion_old, xu.at[1:4, 4:12, 8:24, :], load_sem.at[3]),
        pltpu.make_async_copy(source, own_src, load_sem.at[4]),
        pltpu.make_async_copy(strain_prev, own_strain, load_sem.at[5]),
        pltpu.make_async_copy(body_force, own_bf, load_sem.at[6]),
    ]
    for copy in loads:
        copy.start()

    def clear(ref):
        count = ref.shape[0]

        @pl.loop(0, 18)
        def _(i):
            for f in range(count):
                ref[f, i, 0:8, :] = jnp.zeros((8, 128), F32)
                ref[f, i, 24:32, :] = jnp.zeros((8, 128), F32)

    for ref in (zd, xu, z0, ze, mat, tf, mf, sp, gv, se, mo):
        clear(ref)
    wide = (zd, xu, z0, ze)

    @pl.when(jnp.logical_not(x_lo))
    def _():
        for ref in wide:
            ref[:, 0:4, 8:24, :] = jnp.zeros((ref.shape[0], 4, 16, 128), F32)

    @pl.when(jnp.logical_not(x_hi))
    def _():
        for ref in wide:
            ref[:, 12:16, 8:24, :] = jnp.zeros((ref.shape[0], 4, 16, 128), F32)

    @pl.when(jnp.logical_not(z_lo))
    def _():
        for ref in (pl_zd, pl_xu, pl_z0, pl_ze):
            ref[...] = jnp.zeros(ref.shape, F32)

    @pl.when(jnp.logical_not(z_hi))
    def _():
        for ref in (pr_zd, pr_xu, pr_z0, pr_ze):
            ref[...] = jnp.zeros(ref.shape, F32)

    rows[...] = jnp.zeros((32, 128), F32)
    loads[0].wait()
    loads[1].wait()
    zd[0, 4:12, 8:24, :] = own_zone[...].astype(F32) + 1.0
    zd[1, 4:12, 8:24, :] = own_drain[...].astype(F32)
    loads[2].wait()
    loads[3].wait()

    pl.semaphore_wait(barrier, len(greet))
    if ny > 2 * reach + 1:
        for by in (reach, -reach):
            pl.semaphore_signal(
                known, inc=1, device_id=(gx, turn(gy, by, ny), gz), device_id_type=MESH
            )

    def both(has_lo, has_hi, down, up):
        @pl.when(has_lo)
        def _():
            for copy in down:
                copy.start()

        @pl.when(has_hi)
        def _():
            for copy in up:
                copy.start()

        @pl.when(has_lo)
        def _():
            for copy_up, copy_down in zip(up, down):
                copy_down.wait_send()
                copy_up.wait_recv()

        @pl.when(has_hi)
        def _():
            for copy_up, copy_down in zip(up, down):
                copy_up.wait_send()
                copy_down.wait_recv()

    def send(src, dst, sems, slot, device):
        return pltpu.make_async_remote_copy(
            src_ref=src,
            dst_ref=dst,
            send_sem=sems[0].at[slot],
            recv_sem=sems[1].at[slot],
            device_id=device,
            device_id_type=MESH,
        )

    def exchange(fields, slot):
        down, up = ([], [])
        s = slot
        for ref, n, d, *_ in fields:
            some = pl.ds(0, n)
            down.append(
                send(
                    ref.at[some, pl.ds(4, d), pl.ds(8, 16), :],
                    ref.at[some, pl.ds(12, d), pl.ds(8, 16), :],
                    (xs_sem, xr_sem),
                    s,
                    (gx - 1, gy, gz),
                )
            )
            up.append(
                send(
                    ref.at[some, pl.ds(12 - d, d), pl.ds(8, 16), :],
                    ref.at[some, pl.ds(4 - d, d), pl.ds(8, 16), :],
                    (xs_sem, xr_sem),
                    s + 1,
                    (gx + 1, gy, gz),
                )
            )
            s += 2
        both(x_lo, x_hi, down, up)

        block = lax.broadcasted_iota(jnp.int32, (16, 128), 1) // 8
        down, up = ([], [])
        s = slot
        for ref, n, d, pack, left, right, *_ in fields:
            for f in range(n):
                packed = jnp.zeros((16, 128), F32)
                for i in range(4 - d, 12 + d):
                    turned = pltpu.roll(ref[f, i, 8:24, :], (8 * i + 4) % 128, 1)
                    packed = jnp.where(block == i, turned, packed)
                pack[f] = packed
            down.append(send(pack, right, (zs_sem, zr_sem), s, (gx, gy, gz - 1)))
            up.append(send(pack, left, (zs_sem, zr_sem), s + 1, (gx, gy, gz + 1)))
            s += 2
        both(z_lo, z_hi, down, up)
        low_half = lax.rem(lax.broadcasted_iota(jnp.int32, (16, 128), 1), 8) < 4
        for ref, n, d, pack, left, right, *_ in fields:
            for f in range(n):
                ref[f, L, 8:24, :] = jnp.where(low_half, left[f], pack[f])
                ref[f, R, 8:24, :] = jnp.where(low_half, pack[f], right[f])

        down, up = ([], [])
        s = slot
        for ref, n, d, pack, left, right, ys, yr in fields:
            span = 8 + 2 * d
            ys[0, :, 0:span] = ref[0:n, 4 - d : 12 + d, 8 : 8 + d, :]
            ys[0, :, span : span + 2] = ref[0:n, 16:18, 8 : 8 + d, :]
            ys[1, :, 0:span] = ref[0:n, 4 - d : 12 + d, 24 - d : 24, :]
            ys[1, :, span : span + 2] = ref[0:n, 16:18, 24 - d : 24, :]
            down.append(send(ys.at[0], yr.at[1], (yss_sem, yrs_sem), s, (gx, gy - 1, gz)))
            up.append(send(ys.at[1], yr.at[0], (yss_sem, yrs_sem), s + 1, (gx, gy + 1, gz)))
            s += 2
        both(y_lo, y_hi, down, up)

        @pl.when(y_lo)
        def _():
            for ref, n, d, pack, left, right, ys, yr in fields:
                span = 8 + 2 * d
                ref[0:n, 4 - d : 12 + d, 8 - d : 8, :] = yr[0, :, 0:span]
                ref[0:n, 16:18, 8 - d : 8, :] = yr[0, :, span : span + 2]

        @pl.when(y_hi)
        def _():
            for ref, n, d, pack, left, right, ys, yr in fields:
                span = 8 + 2 * d
                ref[0:n, 4 - d : 12 + d, 24 : 24 + d, :] = yr[1, :, 0:span]
                ref[0:n, 16:18, 24 : 24 + d, :] = yr[1, :, span : span + 2]

    exchange(
        [
            (xu, 4, 1, pk_xu, pl_xu, pr_xu, ys_xu, yr_xu),
            (zd, 2, 4, pk_zd, pl_zd, pr_zd, ys_zd, yr_zd),
        ],
        0,
    )

    def materials(row):
        zone = row.at(zd, 0)
        inside = zone > 0.5
        perm = jnp.zeros(zone.shape, F32)
        lame, shear = (perm, perm)
        for k in range(ZONES):
            hit = zone == k + 1.0
            perm = jnp.where(hit, perm_t[k], perm)
            lame = jnp.where(hit, lame_t[k], lame)
            shear = jnp.where(hit, shear_t[k], shear)
        bulk = jnp.where(inside, lame + 2.0 * shear / 3.0, 1.0)
        row.put(mat, 0, perm)
        row.put(mat, 1, lame + shear)
        row.put(mat, 2, shear)
        row.put(mat, 3, 0.2 + 0.64 / bulk + 2.0 * row.at(zd, 1))

    over_rows(0, 16, materials)

    def faces(row):
        for ref, f in ((tf, 0), (mf, 2)):
            own = row.at(mat, f)
            row.put(ref, 0, harmonic(own, row.xp(mat, f)))
            row.put(ref, 1, harmonic(own, row.yp(mat, f)))
            row.put(ref, 2, harmonic(own, row.zp(mat, f)))
            row.put(ref, 3, harmonic(own, row.zm(mat, f)))

    over_rows(0, 15, faces)

    def six(row, ref):
        return (
            row.at(ref, 0),
            row.xm(ref, 0),
            row.at(ref, 1),
            row.ym(ref, 1),
            row.at(ref, 2),
            row.at(ref, 3),
        )

    def around(row, ref, f):
        return (
            row.xp(ref, f),
            row.xm(ref, f),
            row.yp(ref, f),
            row.ym(ref, f),
            row.zp(ref, f),
            row.zm(ref, f),
        )

    def spread(factors, center, nearby):
        return sum(t * (center - v) for t, v in zip(factors, nearby))

    def diagonals(row):
        total = row.at(mat, 3) + sum(six(row, tf))
        row.put(diag, 0, total)
        row.put(diag, 1, 1.0 / total)
        heft = row.at(mat, 1)
        base = 1.0 + sum(six(row, mf)) + heft
        inside = row.at(mat, 2) > 0.0
        for c, other in enumerate((row.xm(mat, 1), row.ym(mat, 1), row.zm(mat, 1))):
            value = base + other
            row.put(ediag, c, value)
            row.put(ediag, 3 + c, jnp.where(inside, 1.0 / value, 0.0))

    over_rows(1, 15, diagonals)

    def divergence(row, ref, f):
        return (
            row.xp(ref, f)
            - row.at(ref, f)
            + (row.yp(ref, f + 1) - row.at(ref, f + 1))
            + (row.zp(ref, f + 2) - row.at(ref, f + 2))
        )

    def elastic(row, ref, f, g):
        factors = six(row, mf)
        own = row.at(gv, g)
        before = (row.xm(gv, g), row.ym(gv, g), row.zm(gv, g))
        done = []
        for c in range(3):
            center = row.at(ref, f + c)
            done.append(
                center + spread(factors, center, around(row, ref, f + c)) + (before[c] - own)
            )
        return done

    def old_scaled(row):
        row.put(gv, 0, row.at(mat, 1) * divergence(row, xu, 1))

    over_rows(3, 12, old_scaled, strips=(L,))

    for copy in loads[4:]:
        copy.wait()

    def first(row):
        j = row.i - 4
        x0 = row.at(xu, 0)
        nearby = around(row, xu, 0)
        central = 0.5 * (
            row.xp(xu, 1)
            - row.xm(xu, 1)
            + (row.yp(xu, 2) - row.ym(xu, 2))
            + (row.zp(xu, 3) - row.zm(xu, 3))
        )
        residual = (
            own_src[j]
            - 2.0 * row.at(zd, 1) * x0
            - 0.8 * (central - own_strain[j])
            - spread(six(row, tf), x0, nearby)
        )
        row.put(z0, 0, residual * row.at(diag, 1))
        image = elastic(row, xu, 1, 0)
        for c in range(3):
            force = own_bf[c, j] - image[c] - 0.4 * (nearby[2 * c] - nearby[2 * c + 1])
            row.put(ze, c, force * row.at(ediag, 3 + c))

    over_rows(4, 12, first, OWN, ())

    exchange(
        [
            (z0, 1, 4, pk_z0, pl_z0, pr_z0, ys_z0, yr_z0),
            (ze, 3, 2, pk_ze, pl_ze, pr_ze, ys_ze, yr_ze),
        ],
        4,
    )

    def second(row):
        center = row.at(z0, 0)
        image = row.at(mat, 3) * center + spread(six(row, tf), center, around(row, z0, 0))
        row.put(sp, 0, image * row.at(diag, 1))

    over_rows(1, 15, second)

    def basis(row):
        for p, ref in ((1, z0), (2, sp)):
            nearby = around(row, ref, 0)
            for c in range(3):
                force = -0.4 * (nearby[2 * c] - nearby[2 * c + 1])
                row.put(ze, 3 * p + c, force * row.at(ediag, 3 + c))

    over_rows(2, 14, basis)

    def scaled(row):
        heft = row.at(mat, 1)
        for p in range(3):
            row.put(gv, p, heft * divergence(row, ze, 3 * p))

    over_rows(2, 13, scaled)

    def images(row):
        for p in range(3):
            done = elastic(row, ze, 3 * p, p)
            for c in range(3):
                row.put(se, 3 * p + c, done[c] * row.at(ediag, 3 + c))

    over_rows(3, 13, images)

    zero = jnp.zeros((8, 128), F32)
    pairs = [(p, q) for p in range(3) for q in range(p, 3)]

    def pressure_moments(i, sums):
        row = Row(i, OWN, False)
        z, s, d = (row.at(z0, 0), row.at(sp, 0), row.at(diag, 0))
        dz, ds = (d * z, d * s)
        energy = row.at(mat, 3) * s * s
        for f, other in enumerate((row.xp(sp, 0), row.yp(sp, 0), row.zp(sp, 0))):
            gap = s - other
            energy = energy + row.at(tf, f) * gap * gap
        new = (dz * z, dz * s, ds * s, energy)
        return tuple(a + fold(b) for a, b in zip(sums, new))

    def plain_moments(i, sums):
        row = Row(i, OWN, False)
        new = [None] * 18

        def add(k, value):
            new[k] = value if new[k] is None else new[k] + value

        for c in range(3):
            d = row.at(ediag, c)
            g = [row.at(ze, 3 * p + c) for p in range(3)]
            s = [row.at(se, 3 * p + c) for p in range(3)]
            dg = [d * v for v in g]
            ds = [d * v for v in s]
            for k, (p, q) in enumerate(pairs):
                add(k, dg[p] * g[q])
                add(6 + k, dg[p] * s[q])
                add(12 + k, ds[p] * s[q])
        return tuple(a + fold(b) for a, b in zip(sums, new))

    def energy_moments(i, sums):
        row = Row(i, OWN, False)
        new = [jnp.zeros((16, 128), F32)] * 6
        heft = row.at(mat, 1)
        factors = [row.at(mf, f) for f in range(3)]
        div = [None] * 3
        for c in range(3):
            s = [row.at(se, 3 * p + c) for p in range(3)]
            for k, (p, q) in enumerate(pairs):
                new[k] = new[k] + s[p] * s[q]
            for f, pick in enumerate((row.xp, row.yp, row.zp)):
                gap = [pick(se, 3 * p + c) - s[p] for p in range(3)]
                if f == c:
                    div = [g if d is None else d + g for d, g in zip(div, gap)]
                scaled_gap = [factors[f] * g for g in gap]
                for k, (p, q) in enumerate(pairs):
                    new[k] = new[k] + scaled_gap[p] * gap[q]
        for k, (p, q) in enumerate(pairs):
            new[k] = new[k] + heft * div[p] * div[q]
        return tuple(a + fold(b) for a, b in zip(sums, new))

    sums = lax.fori_loop(4, 12, pressure_moments, (zero,) * 4)
    sums += lax.fori_loop(4, 12, plain_moments, (zero,) * 18)
    sums += lax.fori_loop(4, 12, energy_moments, (zero,) * 6)
    for k, value in enumerate(sums):
        rows[k : k + 1, :] = jnp.sum(value, axis=0, keepdims=True)
    eye = lax.broadcasted_iota(jnp.int32, (32, 128), 0) == lax.broadcasted_iota(
        jnp.int32, (32, 128), 1
    )
    column = jnp.sum(rows[...], axis=1, keepdims=True)
    part[0] = jnp.sum(jnp.where(eye, column, 0.0), axis=0, keepdims=True)

    slot = 0
    for stage, (group, got) in enumerate(((group_a, got_a), (group_b, got_b), (group_c, got_c))):
        if stage == 2 and ny > 2 * reach + 1:
            pl.semaphore_wait(known, 2)
        copies = []
        for k, device in enumerate(group):
            copies.append(send(part.at[stage], got.at[k], (rs_sem, rr_sem), slot + k, device))
        slot += len(group)
        for copy in copies:
            copy.start()
        for copy in copies:
            copy.wait()
        total = part[stage]
        for k in range(len(group)):
            total = total + got[k]
        part[stage + 1] = total

    column = jnp.sum(jnp.where(eye, part[3], 0.0), axis=1, keepdims=True)
    m = [column[k : k + 1, :] for k in range(28)]

    def steps(m0, m1, m2, m3):
        alpha = m0 / m1
        gamma = m0 - 2.0 * alpha * m1 + alpha * alpha * m2
        delta = m1 - 2.0 * alpha * m2 + alpha * alpha * m3
        beta = gamma / m0
        step = gamma / (delta - beta * gamma / alpha)
        return (alpha + step * (1.0 + beta), -alpha * step)

    a, b = steps(*m[0:4])

    def quadratic(v):
        return v[0] + 2.0 * (a * v[1] + b * v[2]) + a * a * v[3] + 2.0 * a * b * v[4] + b * b * v[5]

    ea, eb = steps(*[quadratic(m[4 + 6 * k : 10 + 6 * k]) for k in range(4)])

    def moved(row):
        for c in range(3):
            z = row.at(ze, c) + a * row.at(ze, 3 + c) + b * row.at(ze, 6 + c)
            s = row.at(se, c) + a * row.at(se, 3 + c) + b * row.at(se, 6 + c)
            row.put(mo, c, row.at(xu, 1 + c) + ea * z + eb * s)

    over_rows(3, 13, moved)

    def finish(row):
        j = row.i - 4
        press_out[j] = row.at(xu, 0) + a * row.at(z0, 0) + b * row.at(sp, 0)
        for c in range(3):
            motion_out[c, j] = row.at(mo, c)
        strain_out[j] = 0.5 * (
            row.xp(mo, 0)
            - row.xm(mo, 0)
            + (row.yp(mo, 1) - row.ym(mo, 1))
            + (row.zp(mo, 2) - row.zm(mo, 2))
        )

    over_rows(4, 12, finish, OWN, ())


def local_step(sizes, *args):
    nx, ny, nz, cores, xs = sizes

    def field(n):
        return pltpu.VMEM((n, 18, 32, 128), F32)

    def vmem(*shape):
        return pltpu.VMEM(shape, F32)

    moving = ((2, 4), (4, 1), (1, 4), (3, 2))
    packs = [vmem(n, 16, 128) for n, _ in moving]
    y_parts = [vmem(2, n, 10 + 2 * d, d, 128) for n, d in moving]
    group_a, group_b, group_c = (cores * xs, (nx // cores) * (nz // xs), ny)
    sent = group_a + group_b + group_c - 3
    dma = pltpu.SemaphoreType.DMA
    scratch = [
        vmem(8, 16, 128),
        vmem(8, 16, 128),
        vmem(3, 8, 16, 128),
        pltpu.VMEM((8, 16, 128), jnp.int32),
        pltpu.VMEM((8, 16, 128), jnp.int32),
        field(2),
        field(4),
        field(1),
        field(9),
        field(4),
        field(4),
        field(4),
        field(2),
        field(6),
        field(1),
        field(3),
        field(9),
        field(3),
        *packs,
        *packs,
        *packs,
        *y_parts,
        *y_parts,
        vmem(32, 128),
        vmem(4, 1, 128),
        vmem(max(group_a - 1, 1), 1, 128),
        vmem(max(group_b - 1, 1), 1, 128),
        vmem(max(group_c - 1, 1), 1, 128),
        dma((7,)),
        *[dma((8,)) for _ in range(6)],
        dma((max(sent, 1),)),
        dma((max(sent, 1),)),
        pltpu.SemaphoreType.REGULAR,
    ]
    anywhere = pl.BlockSpec(memory_space=pl.ANY)
    scalars = pl.BlockSpec(memory_space=pltpu.SMEM)
    near = pl.BlockSpec(memory_space=pltpu.VMEM)
    return pl.pallas_call(
        functools.partial(kernel, sizes),
        name="biot_step",
        out_shape=(
            jax.ShapeDtypeStruct((8, 16, 128), F32),
            jax.ShapeDtypeStruct((3, 8, 16, 128), F32),
            jax.ShapeDtypeStruct((8, 16, 128), F32),
        ),
        in_specs=[anywhere] * 7 + [scalars] * 3,
        out_specs=(near, near, near),
        scratch_shapes=scratch,
        compiler_params=pltpu.CompilerParams(
            collective_id=0, has_side_effects=True, vmem_limit_bytes=48 * 1024 * 1024
        ),
    )(*args)


def solution(mesh, cores=2, xs=4):
    sizes = (mesh.shape["gx"], mesh.shape["gy"], mesh.shape["gz"], cores, xs)
    scalar = P("gx", "gy", "gz")
    vector = P(None, "gx", "gy", "gz")
    return jax.shard_map(
        functools.partial(local_step, sizes),
        mesh=mesh,
        in_specs=(scalar, scalar, scalar, vector, vector, scalar, scalar, P(), P(), P()),
        out_specs=(scalar, vector, scalar),
        check_vma=False,
    )
```

```python
import functools

import jax
import jax.numpy as jnp
from jax import lax
from jax.experimental import pallas as pl
from jax.experimental.pallas import tpu as pltpu
from jax.sharding import PartitionSpec as P

ZONES = 8
MESH = pl.DeviceIdType.MESH
F32 = jnp.float32
WIN = (4, 24)
OWN = (8, 16)
L, R = (16, 17)


def lanes(rows):
    return lax.broadcasted_iota(jnp.int32, (rows, 128), 1)


class Row:
    def __init__(self, i, window, strip):
        self.i, self.strip = (i, strip)
        self.start, self.count = window
        self.lane = lanes(self.count)

    def at(self, ref, f, dy=0, i=None):
        return ref[f, self.i if i is None else i, pl.ds(self.start + dy, self.count), :]

    def xp(self, ref, f):
        if self.strip:
            return pltpu.roll(self.at(ref, f), 120, 1)
        return self.at(ref, f, i=self.i + 1)

    def xm(self, ref, f):
        if self.strip:
            return pltpu.roll(self.at(ref, f), 8, 1)
        return self.at(ref, f, i=self.i - 1)

    def yp(self, ref, f):
        return self.at(ref, f, dy=1)

    def ym(self, ref, f):
        return self.at(ref, f, dy=-1)

    def zp(self, ref, f):
        turned = pltpu.roll(self.at(ref, f), 127, 1)
        if self.strip:
            return turned
        edge = pltpu.roll(self.at(ref, f, i=R), 123 - 8 * self.i, 1)
        return jnp.where(self.lane == 127, edge, turned)

    def zm(self, ref, f):
        turned = pltpu.roll(self.at(ref, f), 1, 1)
        if self.strip:
            return turned
        edge = pltpu.roll(self.at(ref, f, i=L), 125 - 8 * self.i, 1)
        return jnp.where(self.lane == 0, edge, turned)

    def put(self, ref, f, value):
        ref[f, self.i, pl.ds(self.start, self.count), :] = value


def over_rows(low, high, body, window=WIN, strips=(L, R)):
    @pl.loop(low, high, unroll=min(4, high - low))
    def _(i):
        body(Row(i, window, False))

    if strips:

        @pl.loop(strips[0], strips[-1] + 1, unroll=True)
        def _(i):
            body(Row(i, window, True))


def harmonic(own, beside):
    total = own + beside
    return 2.0 * own * beside / jnp.where(total > 0.0, total, 1.0)


def fold(value):
    return value[0:8] + value[8:16]


def kernel(
    sizes,
    source,
    press_old,
    strain_prev,
    motion_old,
    body_force,
    zones,
    drained,
    perm_h,
    lame_h,
    shear_h,
    press_out,
    motion_out,
    strain_out,
    perm_t,
    lame_t,
    shear_t,
    own_src,
    own_strain,
    own_bf,
    own_zone,
    own_drain,
    zd,
    xu,
    z0,
    ze,
    mat,
    tf,
    mf,
    diag,
    ediag,
    sp,
    gv,
    se,
    mo,
    ys_xu,
    ys_zd,
    ys_z0,
    ys_ze,
    yr_xu,
    yr_zd,
    yr_z0,
    yr_ze,
    strips_1,
    strips_2,
    rows,
    part,
    got_a,
    got_b,
    load_sem,
    hs_sem,
    hr_sem,
    rs_sem,
    rr_sem,
    known,
):
    nx, ny, nz, cores, xs = sizes
    gx, gy, gz = (lax.axis_index("gx"), lax.axis_index("gy"), lax.axis_index("gz"))
    yhs, yls = (nx // cores, nz // xs)
    x_lo, x_hi = (gx > 0, gx < nx - 1)
    y_lo, y_hi = (gy > 0, gy < ny - 1)
    z_lo, z_hi = (gz > 0, gz < nz - 1)
    axes = ((x_lo, x_hi, nx), (y_lo, y_hi, ny), (z_lo, z_hi, nz))

    def turn(value, by, count):
        return lax.rem(value + (by % count), count)

    ways = [
        (dx, dy, dz)
        for dx in (1, -1, 0)
        for dy in (1, -1, 0)
        for dz in (1, -1, 0)
        if dx or dy or dz
    ]
    ways = [w for w in ways if all(count > 1 or not step for step, (_, _, count) in zip(w, axes))]

    def there(way):
        ok = None
        for step, (low, high, _) in zip(way, axes):
            if step:
                side = high if step > 0 else low
                ok = side if ok is None else jnp.logical_and(ok, side)
        return ok

    def device(way):
        return (gx + way[0], gy + way[1], gz + way[2])

    yh, core = (gx // cores, lax.rem(gx, cores))
    yl, xx = (gz // xs, lax.rem(gz, xs))
    group_a = [
        (turn(yh, h, yhs) * cores + core, gy, turn(yl, k, yls) * xs + turn(xx, x, xs))
        for h in range(yhs)
        for k in range(yls)
        for x in range(xs)
        if h or k or x
    ]
    reach = 4
    chained = ny > 2 * reach + 1

    def over_z(k, c):
        return (yh * cores + turn(core, c, cores), turn(gy, k, ny), gz)

    group_b = [over_z(k, c) for k in range(ny) for c in range(cores) if k or c]
    if chained:
        near = [
            over_z(k, c)
            for k in range(-reach, reach + 1)
            for c in range(cores)
            if k or c
        ]
    else:
        near = group_b

    barrier = pltpu.get_barrier_semaphore()
    for way in ways:

        @pl.when(there(way))
        def _(way=way):
            pl.semaphore_signal(barrier, inc=1, device_id=device(way), device_id_type=MESH)

    for other in group_a + near:
        pl.semaphore_signal(barrier, inc=1, device_id=other, device_id_type=MESH)

    loads = [
        pltpu.make_async_copy(src, dst, load_sem.at[k])
        for k, (src, dst) in enumerate(
            (
                (zones, own_zone),
                (drained, own_drain),
                (press_old, xu.at[0, 4:12, 8:24, :]),
                (motion_old, xu.at[1:4, 4:12, 8:24, :]),
                (source, own_src),
                (strain_prev, own_strain),
                (body_force, own_bf),
                (perm_h, perm_t),
                (lame_h, lame_t),
                (shear_h, shear_t),
            )
        )
    ]
    for copy in loads:
        copy.start()

    def send(src, dst, slot, to):
        return pltpu.make_async_remote_copy(
            src_ref=src,
            dst_ref=dst,
            send_sem=hs_sem.at[slot],
            recv_sem=hr_sem.at[slot],
            device_id=to,
            device_id_type=MESH,
        )

    lane = lanes(16)
    block = lane // 8
    quarter = lane // 32
    low_half = lax.rem(lane, 8) < 4

    def side(step):
        return (1, 0) if step > 0 else (0, 1)

    class Exchange:
        def __init__(self, groups, strips, slot):
            self.groups = groups
            self.pk, self.px, self.py, self.pxy, self.rz, self.rxz, self.ryz, self.rxyz = strips
            self.fields = [(ref, f) for ref, n, *_ in groups for f in range(n)]
            self.copies = {}
            for way in ways:
                dx, dy, dz = way
                pairs = []
                if dz:
                    out, come = side(dz)
                    a, b = (side(dx) if dx else (0, 0), side(dy) if dy else (0, 0))
                    if dx and dy:
                        pairs.append((self.pxy.at[a[0], b[0]], self.rxyz.at[come, a[1], b[1]]))
                    elif dx:
                        pairs.append((self.px.at[a[0]], self.rxz.at[come, a[1]]))
                    elif dy:
                        pairs.append((self.py.at[b[0]], self.ryz.at[come, b[1]]))
                    else:
                        pairs.append((self.pk, self.rz.at[come]))
                else:
                    for ref, n, d, ys, yr in groups:
                        if dx:
                            first = 8 - d if dx > 0 else 0
                            put = 0 if dx > 0 else 8 + d
                        if dx and not dy:
                            x_from, x_to = (4 + first, 4 - d + put)
                            some = pl.ds(0, n)
                            pairs.append(
                                (
                                    ref.at[some, pl.ds(x_from, d), pl.ds(8, 16), :],
                                    ref.at[some, pl.ds(x_to, d), pl.ds(8, 16), :],
                                )
                            )
                        elif dx:
                            b = side(dy)
                            pairs.append(
                                (
                                    ys.at[b[0], :, pl.ds(first, d)],
                                    yr.at[b[1], :, pl.ds(put, d)],
                                )
                            )
                        else:
                            b = side(dy)
                            pairs.append((ys.at[b[0]], yr.at[b[1], :, pl.ds(d, 8)]))
                self.copies[way] = [
                    send(src, dst, slot + k, device(way)) for k, (src, dst) in enumerate(pairs)
                ]
                slot += len(pairs)

        def pack(self):
            for ref, n, d, ys, yr in self.groups:
                ys[0] = ref[0:n, 4:12, 8 : 8 + d, :]
                ys[1] = ref[0:n, 4:12, 24 - d : 24, :]
            count = self.px.shape[1]
            across = [[jnp.zeros((16, 128), F32) for _ in range(count)] for _ in range(2)]
            for k, (ref, f) in enumerate(self.fields):
                packed = jnp.zeros((16, 128), F32)
                for i in range(4, 12):
                    turned = pltpu.roll(ref[f, i, 8:24, :], (8 * i + 4) % 128, 1)
                    packed = jnp.where(block == i, turned, packed)
                self.pk[k] = packed
                self.py[0, k] = packed[0:4]
                self.py[1, k] = packed[12:16]
                q, g = (k % 4, k // 4)
                for s, base in ((0, 32), (1, 64)):
                    turned = pltpu.roll(packed, (32 * q - base) % 128, 1)
                    across[s][g] = jnp.where(quarter == q, turned, across[s][g])
            for s in range(2):
                for g in range(count):
                    self.px[s, g] = across[s][g]
                    self.pxy[s, 0, g] = across[s][g][0:4]
                    self.pxy[s, 1, g] = across[s][g][12:16]

        def start(self):
            for way in ways:

                @pl.when(there(way))
                def _(way=way):
                    for copy in self.copies[way]:
                        copy.start()

        def blank(self):
            for s, have in ((0, x_lo), (1, x_hi)):

                @pl.when(jnp.logical_not(have))
                def _(s=s):
                    for ref, n, d, ys, yr in self.groups:
                        ref[0:n, 12 * s : 12 * s + 4, 8:24, :] = jnp.zeros((n, 4, 16, 128), F32)
                        for y in range(2):
                            at = (8 + d) * s
                            yr[y, :, at : at + d] = jnp.zeros((n, d, d, 128), F32)
                    for z in range(2):
                        self.rxz[z, s] = jnp.zeros(self.rxz.shape[2:], F32)
                        self.rxyz[z, s] = jnp.zeros(self.rxyz.shape[2:], F32)

            for s, have in ((0, y_lo), (1, y_hi)):

                @pl.when(jnp.logical_not(have))
                def _(s=s):
                    for z in range(2):
                        self.ryz[z, s] = jnp.zeros(self.ryz.shape[2:], F32)
                        for x in range(2):
                            self.rxyz[z, x, s] = jnp.zeros(self.rxyz.shape[3:], F32)

            for s, have in ((0, z_lo), (1, z_hi)):

                @pl.when(jnp.logical_not(have))
                def _(s=s):
                    for ref in (self.rz, self.rxz, self.ryz, self.rxyz):
                        ref[s] = jnp.zeros(ref.shape[1:], F32)

        def arrived(self, some):
            for way in some:

                @pl.when(there(tuple(-step for step in way)))
                def _(way=way):
                    for copy in self.copies[way]:
                        copy.wait_recv()

        def finish(self):
            self.arrived([way for way in ways if not way[2]])
            for s, have in ((0, y_lo), (1, y_hi)):

                @pl.when(have)
                def _(s=s):
                    for ref, n, d, ys, yr in self.groups:
                        at = 24 if s else 8 - d
                        ref[0:n, 4 - d : 12 + d, at : at + d, :] = yr[s]

            wide = lanes(24) // 8
            for ref, n, d, *_ in self.groups:
                for f in range(n):
                    packed = jnp.zeros((24, 128), F32)
                    for i in range(4 - d, 12 + d):
                        turned = pltpu.roll(ref[f, i, 4:28, :], (8 * i + 4) % 128, 1)
                        packed = jnp.where(wide == i, turned, packed)
                    ref[f, L, 4:28, :] = packed
                    ref[f, R, 4:28, :] = packed
            self.arrived([way for way in ways if way[2]])
            for k, (ref, f) in enumerate(self.fields):
                q, g = (k % 4, k // 4)
                for z, strip in ((0, L), (1, R)):
                    mine = low_half if z == 0 else jnp.logical_not(low_half)

                    def joined(low, middle, high, count):
                        here = lane[0:count]
                        low = pltpu.roll(low, (-32 * q) % 128, 1)
                        high = pltpu.roll(high, (96 - 32 * q) % 128, 1)
                        return jnp.where(here < 32, low, jnp.where(here >= 96, high, middle))

                    for start, count, got in (
                        (8, 16, (self.rxz[z, 0, g], self.rz[z, k], self.rxz[z, 1, g])),
                        (4, 4, (self.rxyz[z, 0, 0, g], self.ryz[z, 0, k], self.rxyz[z, 1, 0, g])),
                        (24, 4, (self.rxyz[z, 0, 1, g], self.ryz[z, 1, k], self.rxyz[z, 1, 1, g])),
                    ):
                        own = ref[f, strip, start : start + count, :]
                        ref[f, strip, start : start + count, :] = jnp.where(
                            mine[0:count], joined(*got, count), own
                        )
            for way in ways:

                @pl.when(there(way))
                def _(way=way):
                    for copy in self.copies[way]:
                        copy.wait_send()

    round_1 = Exchange(
        [(xu, 4, 1, ys_xu, yr_xu), (zd, 2, 4, ys_zd, yr_zd)],
        strips_1,
        0,
    )
    slots_1 = sum(len(c) for c in round_1.copies.values())
    round_2 = Exchange(
        [(z0, 1, 4, ys_z0, yr_z0), (ze, 3, 2, ys_ze, yr_ze)],
        strips_2,
        slots_1,
    )

    for copy in loads[0:4]:
        copy.wait()
    zd[0, 4:12, 8:24, :] = own_zone[...].astype(F32) + 1.0
    zd[1, 4:12, 8:24, :] = own_drain[...].astype(F32)
    round_1.pack()
    greeted = len(group_a) + len(near) - 1
    around_here = None
    for low, high, _ in axes:
        count = 1 + low.astype(jnp.int32) + high.astype(jnp.int32)
        around_here = count if around_here is None else around_here * count
    pl.semaphore_wait(barrier, greeted + around_here)
    round_1.start()
    if chained:
        for by in (reach, -reach):
            pl.semaphore_signal(known, inc=1, device_id=over_z(by, 0), device_id_type=MESH)

    def clear(ref):
        count = ref.shape[0]

        @pl.loop(0, 18, unroll=3)
        def _(i):
            for f in range(count):
                ref[f, i, 0:8, :] = jnp.zeros((8, 128), F32)
                ref[f, i, 24:32, :] = jnp.zeros((8, 128), F32)

    for ref in (zd, xu, z0, ze, mat, tf, mf, sp, gv, se, mo):
        clear(ref)
    round_1.blank()
    round_2.blank()
    rows[...] = jnp.zeros((32, 128), F32)
    for copy in loads[4:]:
        copy.wait()
    round_1.finish()

    def materials(row):
        zone = row.at(zd, 0)
        inside = zone > 0.5
        perm = jnp.zeros(zone.shape, F32)
        lame, shear = (perm, perm)
        for k in range(ZONES):
            hit = zone == k + 1.0
            perm = jnp.where(hit, perm_t[k], perm)
            lame = jnp.where(hit, lame_t[k], lame)
            shear = jnp.where(hit, shear_t[k], shear)
        bulk = jnp.where(inside, lame + 2.0 * shear / 3.0, 1.0)
        row.put(mat, 0, perm)
        row.put(mat, 1, lame + shear)
        row.put(mat, 2, shear)
        row.put(mat, 3, 0.2 + 0.64 / bulk + 2.0 * row.at(zd, 1))

    over_rows(3, 13, materials)

    def faces(row):
        for ref, f in ((tf, 0), (mf, 2)):
            own = row.at(mat, f)
            row.put(ref, 0, harmonic(own, row.xp(mat, f)))
            row.put(ref, 1, harmonic(own, row.yp(mat, f)))
            row.put(ref, 2, harmonic(own, row.zp(mat, f)))
            row.put(ref, 3, harmonic(own, row.zm(mat, f)))

    over_rows(3, 12, faces, strips=())

    def six(row, ref):
        return (
            row.at(ref, 0),
            row.xm(ref, 0),
            row.at(ref, 1),
            row.ym(ref, 1),
            row.at(ref, 2),
            row.at(ref, 3),
        )

    def around(row, ref, f):
        return (
            row.xp(ref, f),
            row.xm(ref, f),
            row.yp(ref, f),
            row.ym(ref, f),
            row.zp(ref, f),
            row.zm(ref, f),
        )

    def spread(factors, center, nearby):
        return sum(t * (center - v) for t, v in zip(factors, nearby))

    def diagonals(row):
        total = row.at(mat, 3) + sum(six(row, tf))
        row.put(diag, 0, total)
        row.put(diag, 1, 1.0 / total)
        heft = row.at(mat, 1)
        base = 1.0 + sum(six(row, mf)) + heft
        inside = row.at(mat, 2) > 0.0
        for c, other in enumerate((row.xm(mat, 1), row.ym(mat, 1), row.zm(mat, 1))):
            value = base + other
            row.put(ediag, c, value)
            row.put(ediag, 3 + c, jnp.where(inside, 1.0 / value, 0.0))

    over_rows(4, 12, diagonals, strips=())

    def divergence(row, ref, f):
        return (
            row.xp(ref, f)
            - row.at(ref, f)
            + (row.yp(ref, f + 1) - row.at(ref, f + 1))
            + (row.zp(ref, f + 2) - row.at(ref, f + 2))
        )

    def elastic(row, ref, f, g):
        factors = six(row, mf)
        own = row.at(gv, g)
        before = (row.xm(gv, g), row.ym(gv, g), row.zm(gv, g))
        done = []
        for c in range(3):
            center = row.at(ref, f + c)
            done.append(
                center + spread(factors, center, around(row, ref, f + c)) + (before[c] - own)
            )
        return done

    def old_scaled(row):
        row.put(gv, 0, row.at(mat, 1) * divergence(row, xu, 1))

    over_rows(3, 12, old_scaled, strips=(L,))

    def first(row):
        j = row.i - 4
        x0 = row.at(xu, 0)
        nearby = around(row, xu, 0)
        central = 0.5 * (
            row.xp(xu, 1)
            - row.xm(xu, 1)
            + (row.yp(xu, 2) - row.ym(xu, 2))
            + (row.zp(xu, 3) - row.zm(xu, 3))
        )
        residual = (
            own_src[j]
            - 2.0 * row.at(zd, 1) * x0
            - 0.8 * (central - own_strain[j])
            - spread(six(row, tf), x0, nearby)
        )
        row.put(z0, 0, residual * row.at(diag, 1))
        image = elastic(row, xu, 1, 0)
        for c in range(3):
            force = own_bf[c, j] - image[c] - 0.4 * (nearby[2 * c] - nearby[2 * c + 1])
            row.put(ze, c, force * row.at(ediag, 3 + c))

    over_rows(4, 12, first, OWN, ())

    round_2.pack()
    round_2.start()
    over_rows(0, 3, materials, strips=())
    over_rows(13, 16, materials, strips=())
    over_rows(0, 3, faces, strips=())
    over_rows(12, 15, faces)
    over_rows(1, 4, diagonals, strips=())
    over_rows(12, 15, diagonals)
    round_2.finish()

    def second(row):
        center = row.at(z0, 0)
        image = row.at(mat, 3) * center + spread(six(row, tf), center, around(row, z0, 0))
        row.put(sp, 0, image * row.at(diag, 1))

    over_rows(1, 15, second)

    def basis(row):
        for p, ref in ((1, z0), (2, sp)):
            nearby = around(row, ref, 0)
            for c in range(3):
                force = -0.4 * (nearby[2 * c] - nearby[2 * c + 1])
                row.put(ze, 3 * p + c, force * row.at(ediag, 3 + c))

    over_rows(2, 14, basis)

    def scaled(row):
        heft = row.at(mat, 1)
        for p in range(3):
            row.put(gv, p, heft * divergence(row, ze, 3 * p))

    over_rows(2, 13, scaled)

    def images(row):
        for p in range(3):
            done = elastic(row, ze, 3 * p, p)
            for c in range(3):
                row.put(se, 3 * p + c, done[c] * row.at(ediag, 3 + c))

    over_rows(3, 13, images)

    zero = jnp.zeros((8, 128), F32)
    pairs = [(p, q) for p in range(3) for q in range(p, 3)]

    def pressure_moments(i, sums):
        row = Row(i, OWN, False)
        z, s, d = (row.at(z0, 0), row.at(sp, 0), row.at(diag, 0))
        dz, ds = (d * z, d * s)
        energy = row.at(mat, 3) * s * s
        for f, other in enumerate((row.xp(sp, 0), row.yp(sp, 0), row.zp(sp, 0))):
            gap = s - other
            energy = energy + row.at(tf, f) * gap * gap
        new = (dz * z, dz * s, ds * s, energy)
        return tuple(a + fold(b) for a, b in zip(sums, new))

    def plain_moments(i, sums):
        row = Row(i, OWN, False)
        new = [None] * 18

        def add(k, value):
            new[k] = value if new[k] is None else new[k] + value

        for c in range(3):
            d = row.at(ediag, c)
            g = [row.at(ze, 3 * p + c) for p in range(3)]
            s = [row.at(se, 3 * p + c) for p in range(3)]
            dg = [d * v for v in g]
            ds = [d * v for v in s]
            for k, (p, q) in enumerate(pairs):
                add(k, dg[p] * g[q])
                add(6 + k, dg[p] * s[q])
                add(12 + k, ds[p] * s[q])
        return tuple(a + fold(b) for a, b in zip(sums, new))

    def energy_moments(i, sums):
        row = Row(i, OWN, False)
        new = [jnp.zeros((16, 128), F32)] * 6
        heft = row.at(mat, 1)
        factors = [row.at(mf, f) for f in range(3)]
        div = [None] * 3
        for c in range(3):
            s = [row.at(se, 3 * p + c) for p in range(3)]
            for k, (p, q) in enumerate(pairs):
                new[k] = new[k] + s[p] * s[q]
            for f, pick in enumerate((row.xp, row.yp, row.zp)):
                gap = [pick(se, 3 * p + c) - s[p] for p in range(3)]
                if f == c:
                    div = [g if d is None else d + g for d, g in zip(div, gap)]
                scaled_gap = [factors[f] * g for g in gap]
                for k, (p, q) in enumerate(pairs):
                    new[k] = new[k] + scaled_gap[p] * gap[q]
        for k, (p, q) in enumerate(pairs):
            new[k] = new[k] + heft * div[p] * div[q]
        return tuple(a + fold(b) for a, b in zip(sums, new))

    sums = lax.fori_loop(4, 12, pressure_moments, (zero,) * 4, unroll=4)
    sums += lax.fori_loop(4, 12, plain_moments, (zero,) * 18, unroll=4)
    sums += lax.fori_loop(4, 12, energy_moments, (zero,) * 6, unroll=4)
    for k, value in enumerate(sums):
        rows[k : k + 1, :] = jnp.sum(value, axis=0, keepdims=True)
    eye = lax.broadcasted_iota(jnp.int32, (32, 128), 0) == lax.broadcasted_iota(
        jnp.int32, (32, 128), 1
    )
    column = jnp.sum(rows[...], axis=1, keepdims=True)
    part[0] = jnp.sum(jnp.where(eye, column, 0.0), axis=0, keepdims=True)

    slot = 0
    for stage, (group, got) in enumerate(((group_a, got_a), (group_b, got_b))):
        if stage == 1 and chained:
            pl.semaphore_wait(known, 2)
        copies = [
            pltpu.make_async_remote_copy(
                src_ref=part.at[stage],
                dst_ref=got.at[k],
                send_sem=rs_sem.at[slot + k],
                recv_sem=rr_sem.at[slot + k],
                device_id=other,
                device_id_type=MESH,
            )
            for k, other in enumerate(group)
        ]
        slot += len(group)
        for copy in copies:
            copy.start()
        for copy in copies:
            copy.wait()
        total = part[stage]
        for k in range(len(group)):
            total = total + got[k]
        part[stage + 1] = total

    column = jnp.sum(jnp.where(eye, part[2], 0.0), axis=1, keepdims=True)
    m = [column[k : k + 1, :] for k in range(28)]

    def steps(m0, m1, m2, m3):
        alpha = m0 / m1
        gamma = m0 - 2.0 * alpha * m1 + alpha * alpha * m2
        delta = m1 - 2.0 * alpha * m2 + alpha * alpha * m3
        beta = gamma / m0
        step = gamma / (delta - beta * gamma / alpha)
        return (alpha + step * (1.0 + beta), -alpha * step)

    a, b = steps(*m[0:4])

    def quadratic(v):
        return v[0] + 2.0 * (a * v[1] + b * v[2]) + a * a * v[3] + 2.0 * a * b * v[4] + b * b * v[5]

    ea, eb = steps(*[quadratic(m[4 + 6 * k : 10 + 6 * k]) for k in range(4)])

    def moved(row):
        for c in range(3):
            z = row.at(ze, c) + a * row.at(ze, 3 + c) + b * row.at(ze, 6 + c)
            s = row.at(se, c) + a * row.at(se, 3 + c) + b * row.at(se, 6 + c)
            row.put(mo, c, row.at(xu, 1 + c) + ea * z + eb * s)

    over_rows(3, 13, moved)

    def finish(row):
        j = row.i - 4
        press_out[j] = row.at(xu, 0) + a * row.at(z0, 0) + b * row.at(sp, 0)
        for c in range(3):
            motion_out[c, j] = row.at(mo, c)
        strain_out[j] = 0.5 * (
            row.xp(mo, 0)
            - row.xm(mo, 0)
            + (row.yp(mo, 1) - row.ym(mo, 1))
            + (row.zp(mo, 2) - row.zm(mo, 2))
        )

    over_rows(4, 12, finish, OWN, ())


def local_step(sizes, *args):
    nx, ny, nz, cores, xs = sizes

    def field(n):
        return pltpu.VMEM((n, 18, 32, 128), F32)

    def vmem(*shape):
        return pltpu.VMEM(shape, F32)

    def strips(n):
        g = -(-n // 4)
        return (
            vmem(n, 16, 128),
            vmem(2, g, 16, 128),
            vmem(2, n, 4, 128),
            vmem(2, 2, g, 4, 128),
            vmem(2, n, 16, 128),
            vmem(2, 2, g, 16, 128),
            vmem(2, 2, n, 4, 128),
            vmem(2, 2, 2, g, 4, 128),
        )

    moving = ((4, 1), (2, 4), (1, 4), (3, 2))
    count_a, count_b = (nx // cores * nz - 1, ny * cores - 1)
    sent = max(count_a + count_b, 1)
    dma = pltpu.SemaphoreType.DMA
    scratch = [
        *[pltpu.SMEM((ZONES,), F32) for _ in range(3)],
        vmem(8, 16, 128),
        vmem(8, 16, 128),
        vmem(3, 8, 16, 128),
        pltpu.VMEM((8, 16, 128), jnp.int32),
        pltpu.VMEM((8, 16, 128), jnp.int32),
        field(2),
        field(4),
        field(1),
        field(9),
        field(4),
        field(4),
        field(4),
        field(2),
        field(6),
        field(1),
        field(3),
        field(9),
        field(3),
        *[vmem(2, n, 8, d, 128) for n, d in moving],
        *[vmem(2, n, 8 + 2 * d, d, 128) for n, d in moving],
        strips(6),
        strips(4),
        vmem(32, 128),
        vmem(3, 1, 128),
        vmem(max(count_a, 1), 1, 128),
        vmem(max(count_b, 1), 1, 128),
        dma((10,)),
        dma((68,)),
        dma((68,)),
        dma((sent,)),
        dma((sent,)),
        pltpu.SemaphoreType.REGULAR,
    ]
    far = pl.BlockSpec(memory_space=pltpu.HBM)
    near = pl.BlockSpec(memory_space=pltpu.VMEM)
    return pl.pallas_call(
        functools.partial(kernel, sizes),
        name="biot_step",
        out_shape=(
            jax.ShapeDtypeStruct((8, 16, 128), F32),
            jax.ShapeDtypeStruct((3, 8, 16, 128), F32),
            jax.ShapeDtypeStruct((8, 16, 128), F32),
        ),
        in_specs=[far] * 10,
        out_specs=(near, near, near),
        scratch_shapes=scratch,
        compiler_params=pltpu.CompilerParams(
            collective_id=0, has_side_effects=True, vmem_limit_bytes=67043328
        ),
    )(*args)


def solution(mesh, cores=2, xs=4):
    sizes = (mesh.shape["gx"], mesh.shape["gy"], mesh.shape["gz"], cores, xs)
    scalar = P("gx", "gy", "gz")
    vector = P(None, "gx", "gy", "gz")
    return jax.shard_map(
        functools.partial(local_step, sizes),
        mesh=mesh,
        in_specs=(scalar, scalar, scalar, vector, vector, scalar, scalar, P(), P(), P()),
        out_specs=(scalar, vector, scalar),
        check_vma=False,
    )
```

```python
import functools

import jax
import jax.numpy as jnp
from jax import lax
from jax.experimental import pallas as pl
from jax.experimental.pallas import tpu as pltpu
from jax.sharding import PartitionSpec as P

ZONES = 8
MESH = pl.DeviceIdType.MESH
F32 = jnp.float32
WIN = (4, 24)
OWN = (8, 16)
L, R = (16, 17)


def lanes(rows):
    return lax.broadcasted_iota(jnp.int32, (rows, 128), 1)


class Row:
    def __init__(self, i, window, strip):
        self.i, self.strip = (i, strip)
        self.start, self.count = window
        self.lane = lanes(self.count)

    def at(self, ref, f, dy=0, i=None):
        return ref[f, self.i if i is None else i, pl.ds(self.start + dy, self.count), :]

    def xp(self, ref, f):
        if self.strip:
            return pltpu.roll(self.at(ref, f), 120, 1)
        return self.at(ref, f, i=self.i + 1)

    def xm(self, ref, f):
        if self.strip:
            return pltpu.roll(self.at(ref, f), 8, 1)
        return self.at(ref, f, i=self.i - 1)

    def yp(self, ref, f):
        return self.at(ref, f, dy=1)

    def ym(self, ref, f):
        return self.at(ref, f, dy=-1)

    def zp(self, ref, f):
        turned = pltpu.roll(self.at(ref, f), 127, 1)
        if self.strip:
            return turned
        edge = pltpu.roll(self.at(ref, f, i=R), 123 - 8 * self.i, 1)
        return jnp.where(self.lane == 127, edge, turned)

    def zm(self, ref, f):
        turned = pltpu.roll(self.at(ref, f), 1, 1)
        if self.strip:
            return turned
        edge = pltpu.roll(self.at(ref, f, i=L), 125 - 8 * self.i, 1)
        return jnp.where(self.lane == 0, edge, turned)

    def put(self, ref, f, value):
        ref[f, self.i, pl.ds(self.start, self.count), :] = value


def over_rows(low, high, body, window=WIN, strips=(L, R)):
    @pl.loop(low, high, unroll=min(4, high - low))
    def _(i):
        body(Row(i, window, False))

    if strips:

        @pl.loop(strips[0], strips[-1] + 1, unroll=True)
        def _(i):
            body(Row(i, window, True))


def harmonic(own, beside):
    total = own + beside
    return 2.0 * own * beside / jnp.where(total > 0.0, total, 1.0)


def fold(value):
    return value[0:8] + value[8:16]


def kernel(
    sizes,
    source,
    press_old,
    strain_prev,
    motion_old,
    body_force,
    zones,
    drained,
    perm_h,
    lame_h,
    shear_h,
    press_out,
    motion_out,
    strain_out,
    perm_t,
    lame_t,
    shear_t,
    own_src,
    own_strain,
    own_bf,
    own_zone,
    own_drain,
    zd,
    xu,
    z0,
    ze,
    mat,
    tf,
    mf,
    diag,
    ediag,
    sp,
    gv,
    se,
    cd,
    ys_xu,
    ys_zd,
    ys_z0,
    ys_ze,
    yr_xu,
    yr_zd,
    yr_z0,
    yr_ze,
    strips_1,
    strips_2,
    rows,
    part,
    got_a,
    got_b,
    load_sem,
    hs_sem,
    hr_sem,
    rs_sem,
    rr_sem,
    known,
):
    nx, ny, nz, cores, xs = sizes
    gx, gy, gz = (lax.axis_index("gx"), lax.axis_index("gy"), lax.axis_index("gz"))
    yhs, yls = (nx // cores, nz // xs)
    x_lo, x_hi = (gx > 0, gx < nx - 1)
    y_lo, y_hi = (gy > 0, gy < ny - 1)
    z_lo, z_hi = (gz > 0, gz < nz - 1)
    axes = ((x_lo, x_hi, nx), (y_lo, y_hi, ny), (z_lo, z_hi, nz))

    def turn(value, by, count):
        return lax.rem(value + (by % count), count)

    ways = [
        (dx, dy, dz)
        for dx in (1, -1, 0)
        for dy in (1, -1, 0)
        for dz in (1, -1, 0)
        if dx or dy or dz
    ]
    ways = [w for w in ways if all(count > 1 or not step for step, (_, _, count) in zip(w, axes))]

    def there(way):
        ok = None
        for step, (low, high, _) in zip(way, axes):
            if step:
                side = high if step > 0 else low
                ok = side if ok is None else jnp.logical_and(ok, side)
        return ok

    def device(way):
        return (gx + way[0], gy + way[1], gz + way[2])

    yh, core = (gx // cores, lax.rem(gx, cores))
    yl, xx = (gz // xs, lax.rem(gz, xs))

    def far(step, count):
        return -min(step % count, -step % count)

    steps_a = [(h, k, x) for h in range(yhs) for k in range(yls) for x in range(xs) if h or k or x]
    steps_a.sort(key=lambda t: far(t[0] * yls + t[1], yhs * yls) + far(t[2], xs))
    group_a = [
        (turn(yh, h, yhs) * cores + core, gy, turn(yl, k, yls) * xs + turn(xx, x, xs))
        for h, k, x in steps_a
    ]
    reach = 4
    chained = ny > 2 * reach + 1

    def over_z(k, c):
        return (yh * cores + turn(core, c, cores), turn(gy, k, ny), gz)

    steps_b = [(k, c) for k in range(ny) for c in range(cores) if k or c]
    steps_b.sort(key=lambda t: far(t[0], ny))
    group_b = [over_z(k, c) for k, c in steps_b]
    if chained:
        near = [
            over_z(k, c)
            for k in range(-reach, reach + 1)
            for c in range(cores)
            if k or c
        ]
    else:
        near = group_b

    loads = [
        pltpu.make_async_copy(src, dst, load_sem.at[k])
        for k, (src, dst) in enumerate(
            (
                (zones, own_zone),
                (drained, own_drain),
                (press_old, xu.at[0, 4:12, 8:24, :]),
                (motion_old, xu.at[1:4, 4:12, 8:24, :]),
                (source, own_src),
                (strain_prev, own_strain),
                (body_force, own_bf),
                (perm_h, perm_t),
                (lame_h, lame_t),
                (shear_h, shear_t),
            )
        )
    ]
    for copy in loads:
        copy.start()

    barrier = pltpu.get_barrier_semaphore()
    for way in ways:

        @pl.when(there(way))
        def _(way=way):
            pl.semaphore_signal(barrier, inc=1, device_id=device(way), device_id_type=MESH)

    for other in group_a + near:
        pl.semaphore_signal(barrier, inc=1, device_id=other, device_id_type=MESH)

    def send(src, dst, slot, to):
        return pltpu.make_async_remote_copy(
            src_ref=src,
            dst_ref=dst,
            send_sem=hs_sem.at[slot],
            recv_sem=hr_sem.at[slot],
            device_id=to,
            device_id_type=MESH,
        )

    lane = lanes(16)
    block = lane // 8
    quarter = lane // 32
    low_half = lax.rem(lane, 8) < 4

    def side(step):
        return (1, 0) if step > 0 else (0, 1)

    class Exchange:
        def __init__(self, groups, strips, slot):
            self.groups = groups
            self.pk, self.px, self.py, self.pxy, self.rz, self.rxz, self.ryz, self.rxyz = strips
            self.fields = [(ref, f) for ref, n, *_ in groups for f in range(n)]
            self.copies = {}
            for way in ways:
                dx, dy, dz = way
                pairs = []
                if dz:
                    out, come = side(dz)
                    a, b = (side(dx) if dx else (0, 0), side(dy) if dy else (0, 0))
                    if dx and dy:
                        pairs.append((self.pxy.at[a[0], b[0]], self.rxyz.at[come, a[1], b[1]]))
                    elif dx:
                        pairs.append((self.px.at[a[0]], self.rxz.at[come, a[1]]))
                    elif dy:
                        pairs.append((self.py.at[b[0]], self.ryz.at[come, b[1]]))
                    else:
                        pairs.append((self.pk, self.rz.at[come]))
                else:
                    for ref, n, d, ys, yr in groups:
                        if dx:
                            first = 8 - d if dx > 0 else 0
                            put = 0 if dx > 0 else 8 + d
                        if dx and not dy:
                            x_from, x_to = (4 + first, 4 - d + put)
                            some = pl.ds(0, n)
                            pairs.append(
                                (
                                    ref.at[some, pl.ds(x_from, d), pl.ds(8, 16), :],
                                    ref.at[some, pl.ds(x_to, d), pl.ds(8, 16), :],
                                )
                            )
                        elif dx:
                            b = side(dy)
                            pairs.append(
                                (
                                    ys.at[b[0], :, pl.ds(first, d)],
                                    yr.at[b[1], :, pl.ds(put, d)],
                                )
                            )
                        else:
                            b = side(dy)
                            pairs.append((ys.at[b[0]], yr.at[b[1], :, pl.ds(d, 8)]))
                self.copies[way] = [
                    send(src, dst, slot + k, device(way)) for k, (src, dst) in enumerate(pairs)
                ]
                slot += len(pairs)

        def pack(self):
            for ref, n, d, ys, yr in self.groups:
                ys[0] = ref[0:n, 4:12, 8 : 8 + d, :]
                ys[1] = ref[0:n, 4:12, 24 - d : 24, :]
            count = self.px.shape[1]
            across = [[jnp.zeros((16, 128), F32) for _ in range(count)] for _ in range(2)]
            for k, (ref, f) in enumerate(self.fields):
                packed = jnp.zeros((16, 128), F32)
                for i in range(4, 12):
                    turned = pltpu.roll(ref[f, i, 8:24, :], (8 * i + 4) % 128, 1)
                    packed = jnp.where(block == i, turned, packed)
                self.pk[k] = packed
                self.py[0, k] = packed[0:4]
                self.py[1, k] = packed[12:16]
                q, g = (k % 4, k // 4)
                for s, base in ((0, 32), (1, 64)):
                    turned = pltpu.roll(packed, (32 * q - base) % 128, 1)
                    across[s][g] = jnp.where(quarter == q, turned, across[s][g])
            for s in range(2):
                for g in range(count):
                    self.px[s, g] = across[s][g]
                    self.pxy[s, 0, g] = across[s][g][0:4]
                    self.pxy[s, 1, g] = across[s][g][12:16]

        def start(self):
            for way in ways:

                @pl.when(there(way))
                def _(way=way):
                    for copy in self.copies[way]:
                        copy.start()

        def blank(self):
            for s, have in ((0, x_lo), (1, x_hi)):

                @pl.when(jnp.logical_not(have))
                def _(s=s):
                    for ref, n, d, ys, yr in self.groups:
                        ref[0:n, 12 * s : 12 * s + 4, 8:24, :] = jnp.zeros((n, 4, 16, 128), F32)
                        for y in range(2):
                            at = (8 + d) * s
                            yr[y, :, at : at + d] = jnp.zeros((n, d, d, 128), F32)
                    for z in range(2):
                        self.rxz[z, s] = jnp.zeros(self.rxz.shape[2:], F32)
                        self.rxyz[z, s] = jnp.zeros(self.rxyz.shape[2:], F32)

            for s, have in ((0, y_lo), (1, y_hi)):

                @pl.when(jnp.logical_not(have))
                def _(s=s):
                    for z in range(2):
                        self.ryz[z, s] = jnp.zeros(self.ryz.shape[2:], F32)
                        for x in range(2):
                            self.rxyz[z, x, s] = jnp.zeros(self.rxyz.shape[3:], F32)

            for s, have in ((0, z_lo), (1, z_hi)):

                @pl.when(jnp.logical_not(have))
                def _(s=s):
                    for ref in (self.rz, self.rxz, self.ryz, self.rxyz):
                        ref[s] = jnp.zeros(ref.shape[1:], F32)

        def arrived(self, some):
            for way in some:

                @pl.when(there(tuple(-step for step in way)))
                def _(way=way):
                    for copy in self.copies[way]:
                        copy.wait_recv()

        def finish(self):
            self.arrived([way for way in ways if not way[2]])
            for s, have in ((0, y_lo), (1, y_hi)):

                @pl.when(have)
                def _(s=s):
                    for ref, n, d, ys, yr in self.groups:
                        at = 24 if s else 8 - d
                        ref[0:n, 4 - d : 12 + d, at : at + d, :] = yr[s]

            wide = lanes(24) // 8
            for ref, n, d, *_ in self.groups:
                for f in range(n):
                    packed = jnp.zeros((24, 128), F32)
                    for i in range(4 - d, 12 + d):
                        turned = pltpu.roll(ref[f, i, 4:28, :], (8 * i + 4) % 128, 1)
                        packed = jnp.where(wide == i, turned, packed)
                    ref[f, L, 4:28, :] = packed
                    ref[f, R, 4:28, :] = packed
            self.arrived([way for way in ways if way[2]])
            for k, (ref, f) in enumerate(self.fields):
                q, g = (k % 4, k // 4)
                for z, strip in ((0, L), (1, R)):
                    mine = low_half if z == 0 else jnp.logical_not(low_half)

                    def joined(low, middle, high, count):
                        here = lane[0:count]
                        low = pltpu.roll(low, (-32 * q) % 128, 1)
                        high = pltpu.roll(high, (96 - 32 * q) % 128, 1)
                        return jnp.where(here < 32, low, jnp.where(here >= 96, high, middle))

                    for start, count, got in (
                        (8, 16, (self.rxz[z, 0, g], self.rz[z, k], self.rxz[z, 1, g])),
                        (4, 4, (self.rxyz[z, 0, 0, g], self.ryz[z, 0, k], self.rxyz[z, 1, 0, g])),
                        (24, 4, (self.rxyz[z, 0, 1, g], self.ryz[z, 1, k], self.rxyz[z, 1, 1, g])),
                    ):
                        own = ref[f, strip, start : start + count, :]
                        ref[f, strip, start : start + count, :] = jnp.where(
                            mine[0:count], joined(*got, count), own
                        )
            for way in ways:

                @pl.when(there(way))
                def _(way=way):
                    for copy in self.copies[way]:
                        copy.wait_send()

    round_1 = Exchange(
        [(xu, 4, 1, ys_xu, yr_xu), (zd, 2, 4, ys_zd, yr_zd)],
        strips_1,
        0,
    )
    slots_1 = sum(len(c) for c in round_1.copies.values())
    round_2 = Exchange(
        [(z0, 1, 4, ys_z0, yr_z0), (ze, 3, 2, ys_ze, yr_ze)],
        strips_2,
        slots_1,
    )

    for copy in loads[0:4]:
        copy.wait()
    zd[0, 4:12, 8:24, :] = own_zone[...].astype(F32) + 1.0
    zd[1, 4:12, 8:24, :] = own_drain[...].astype(F32)
    round_1.pack()
    greeted = len(group_a) + len(near) - 1
    around_here = None
    for low, high, _ in axes:
        count = 1 + low.astype(jnp.int32) + high.astype(jnp.int32)
        around_here = count if around_here is None else around_here * count
    pl.semaphore_wait(barrier, greeted + around_here)
    round_1.start()
    if chained:
        for by in (reach, -reach):
            pl.semaphore_signal(known, inc=1, device_id=over_z(by, 0), device_id_type=MESH)

    def clear(ref):
        count = ref.shape[0]

        @pl.loop(0, 18, unroll=3)
        def _(i):
            for f in range(count):
                ref[f, i, 0:8, :] = jnp.zeros((8, 128), F32)
                ref[f, i, 24:32, :] = jnp.zeros((8, 128), F32)

    for ref in (zd, xu, z0, ze, mat, tf, mf, sp, gv, se):
        clear(ref)
    round_1.blank()
    round_2.blank()
    rows[...] = jnp.zeros((32, 128), F32)
    for copy in loads[4:]:
        copy.wait()
    round_1.finish()

    def materials(row):
        zone = row.at(zd, 0)
        inside = zone > 0.5
        perm = jnp.zeros(zone.shape, F32)
        lame, shear = (perm, perm)
        for k in range(ZONES):
            hit = zone == k + 1.0
            perm = jnp.where(hit, perm_t[k], perm)
            lame = jnp.where(hit, lame_t[k], lame)
            shear = jnp.where(hit, shear_t[k], shear)
        bulk = jnp.where(inside, lame + 2.0 * shear / 3.0, 1.0)
        row.put(mat, 0, perm)
        row.put(mat, 1, lame + shear)
        row.put(mat, 2, shear)
        row.put(mat, 3, 0.2 + 0.64 / bulk + 2.0 * row.at(zd, 1))

    over_rows(3, 13, materials)

    def faces(row):
        for ref, f in ((tf, 0), (mf, 2)):
            own = row.at(mat, f)
            row.put(ref, 0, harmonic(own, row.xp(mat, f)))
            row.put(ref, 1, harmonic(own, row.yp(mat, f)))
            row.put(ref, 2, harmonic(own, row.zp(mat, f)))
            row.put(ref, 3, harmonic(own, row.zm(mat, f)))

    over_rows(3, 12, faces, strips=())

    def six(row, ref):
        return (
            row.at(ref, 0),
            row.xm(ref, 0),
            row.at(ref, 1),
            row.ym(ref, 1),
            row.at(ref, 2),
            row.at(ref, 3),
        )

    def around(row, ref, f):
        return (
            row.xp(ref, f),
            row.xm(ref, f),
            row.yp(ref, f),
            row.ym(ref, f),
            row.zp(ref, f),
            row.zm(ref, f),
        )

    def spread(factors, center, nearby):
        return sum(t * (center - v) for t, v in zip(factors, nearby))

    def diagonals(row):
        total = row.at(mat, 3) + sum(six(row, tf))
        row.put(diag, 0, total)
        row.put(diag, 1, 1.0 / total)
        heft = row.at(mat, 1)
        base = 1.0 + sum(six(row, mf)) + heft
        inside = row.at(mat, 2) > 0.0
        for c, other in enumerate((row.xm(mat, 1), row.ym(mat, 1), row.zm(mat, 1))):
            value = base + other
            row.put(ediag, c, value)
            row.put(ediag, 3 + c, jnp.where(inside, 1.0 / value, 0.0))

    over_rows(4, 12, diagonals, strips=())

    def divergence(row, ref, f):
        return (
            row.xp(ref, f)
            - row.at(ref, f)
            + (row.yp(ref, f + 1) - row.at(ref, f + 1))
            + (row.zp(ref, f + 2) - row.at(ref, f + 2))
        )

    def elastic(row, ref, f, g):
        factors = six(row, mf)
        own = row.at(gv, g)
        before = (row.xm(gv, g), row.ym(gv, g), row.zm(gv, g))
        done = []
        for c in range(3):
            center = row.at(ref, f + c)
            done.append(
                center + spread(factors, center, around(row, ref, f + c)) + (before[c] - own)
            )
        return done

    def old_scaled(row):
        row.put(gv, 0, row.at(mat, 1) * divergence(row, xu, 1))

    over_rows(3, 12, old_scaled, strips=(L,))

    def first(row):
        j = row.i - 4
        x0 = row.at(xu, 0)
        nearby = around(row, xu, 0)
        central = 0.5 * (
            row.xp(xu, 1)
            - row.xm(xu, 1)
            + (row.yp(xu, 2) - row.ym(xu, 2))
            + (row.zp(xu, 3) - row.zm(xu, 3))
        )
        residual = (
            own_src[j]
            - 2.0 * row.at(zd, 1) * x0
            - 0.8 * (central - own_strain[j])
            - spread(six(row, tf), x0, nearby)
        )
        row.put(z0, 0, residual * row.at(diag, 1))
        image = elastic(row, xu, 1, 0)
        for c in range(3):
            force = own_bf[c, j] - image[c] - 0.4 * (nearby[2 * c] - nearby[2 * c + 1])
            row.put(ze, c, force * row.at(ediag, 3 + c))

    over_rows(4, 12, first, OWN, ())

    round_2.pack()
    round_2.start()
    over_rows(0, 3, materials, strips=())
    over_rows(13, 16, materials, strips=())
    over_rows(0, 3, faces, strips=())
    over_rows(12, 15, faces)
    over_rows(1, 4, diagonals, strips=())
    over_rows(12, 15, diagonals)
    round_2.finish()

    def second(row):
        center = row.at(z0, 0)
        image = row.at(mat, 3) * center + spread(six(row, tf), center, around(row, z0, 0))
        row.put(sp, 0, image * row.at(diag, 1))

    over_rows(1, 15, second)

    def basis(row):
        for p, ref in ((1, z0), (2, sp)):
            nearby = around(row, ref, 0)
            for c in range(3):
                force = -0.4 * (nearby[2 * c] - nearby[2 * c + 1])
                row.put(ze, 3 * p + c, force * row.at(ediag, 3 + c))

    over_rows(2, 14, basis)

    def scaled(row):
        heft = row.at(mat, 1)
        for p in range(3):
            row.put(gv, p, heft * divergence(row, ze, 3 * p))

    over_rows(2, 13, scaled)

    def images(row):
        for p in range(3):
            done = elastic(row, ze, 3 * p, p)
            for c in range(3):
                row.put(se, 3 * p + c, done[c] * row.at(ediag, 3 + c))

    over_rows(3, 13, images)

    zero = jnp.zeros((8, 128), F32)
    pairs = [(p, q) for p in range(3) for q in range(p, 3)]

    def pressure_moments(i, sums):
        row = Row(i, OWN, False)
        z, s, d = (row.at(z0, 0), row.at(sp, 0), row.at(diag, 0))
        dz, ds = (d * z, d * s)
        energy = row.at(mat, 3) * s * s
        for f, other in enumerate((row.xp(sp, 0), row.yp(sp, 0), row.zp(sp, 0))):
            gap = s - other
            energy = energy + row.at(tf, f) * gap * gap
        new = (dz * z, dz * s, ds * s, energy)
        return tuple(a + fold(b) for a, b in zip(sums, new))

    def plain_moments(i, sums):
        row = Row(i, OWN, False)
        new = [None] * 18

        def add(k, value):
            new[k] = value if new[k] is None else new[k] + value

        for c in range(3):
            d = row.at(ediag, c)
            g = [row.at(ze, 3 * p + c) for p in range(3)]
            s = [row.at(se, 3 * p + c) for p in range(3)]
            dg = [d * v for v in g]
            ds = [d * v for v in s]
            for k, (p, q) in enumerate(pairs):
                add(k, dg[p] * g[q])
                add(6 + k, dg[p] * s[q])
                add(12 + k, ds[p] * s[q])
        return tuple(a + fold(b) for a, b in zip(sums, new))

    def energy_moments(i, sums):
        row = Row(i, OWN, False)
        new = [jnp.zeros((16, 128), F32)] * 6
        heft = row.at(mat, 1)
        factors = [row.at(mf, f) for f in range(3)]
        div = [None] * 3
        for c in range(3):
            s = [row.at(se, 3 * p + c) for p in range(3)]
            for k, (p, q) in enumerate(pairs):
                new[k] = new[k] + s[p] * s[q]
            for f, pick in enumerate((row.xp, row.yp, row.zp)):
                gap = [pick(se, 3 * p + c) - s[p] for p in range(3)]
                if f == c:
                    div = [g if d is None else d + g for d, g in zip(div, gap)]
                scaled_gap = [factors[f] * g for g in gap]
                for k, (p, q) in enumerate(pairs):
                    new[k] = new[k] + scaled_gap[p] * gap[q]
        for k, (p, q) in enumerate(pairs):
            new[k] = new[k] + heft * div[p] * div[q]
        return tuple(a + fold(b) for a, b in zip(sums, new))

    sums = lax.fori_loop(4, 12, pressure_moments, (zero,) * 4, unroll=4)
    sums += lax.fori_loop(4, 12, plain_moments, (zero,) * 18, unroll=4)
    sums += lax.fori_loop(4, 12, energy_moments, (zero,) * 6, unroll=4)
    for k, value in enumerate(sums):
        rows[k : k + 1, :] = jnp.sum(value, axis=0, keepdims=True)
    eye = lax.broadcasted_iota(jnp.int32, (32, 128), 0) == lax.broadcasted_iota(
        jnp.int32, (32, 128), 1
    )
    column = jnp.sum(rows[...], axis=1, keepdims=True)
    part[0] = jnp.sum(jnp.where(eye, column, 0.0), axis=0, keepdims=True)

    def strains(row):
        for k, (ref, f) in enumerate(
            ((xu, 1), (ze, 0), (ze, 3), (ze, 6), (se, 0), (se, 3), (se, 6))
        ):
            cd[k, row.i - 4] = 0.5 * (
                row.xp(ref, f)
                - row.xm(ref, f)
                + (row.yp(ref, f + 1) - row.ym(ref, f + 1))
                + (row.zp(ref, f + 2) - row.zm(ref, f + 2))
            )

    slot = 0
    sent = []
    for stage, (group, got) in enumerate(((group_a, got_a), (group_b, got_b))):
        if stage == 1 and chained:
            pl.semaphore_wait(known, 2)
        copies = [
            pltpu.make_async_remote_copy(
                src_ref=part.at[stage],
                dst_ref=got.at[k],
                send_sem=rs_sem.at[slot + k],
                recv_sem=rr_sem.at[slot + k],
                device_id=other,
                device_id_type=MESH,
            )
            for k, other in enumerate(group)
        ]
        slot += len(group)
        for copy in copies:
            copy.start()
        sent += copies
        if stage == 0:
            over_rows(4, 12, strains, OWN, ())
        for copy in copies:
            copy.wait_recv()
        total = part[stage]
        for k in range(len(group)):
            total = total + got[k]
        part[stage + 1] = total

    column = jnp.sum(jnp.where(eye, part[2], 0.0), axis=1, keepdims=True)
    m = [column[k : k + 1, :] for k in range(28)]

    def steps(m0, m1, m2, m3):
        alpha = m0 / m1
        gamma = m0 - 2.0 * alpha * m1 + alpha * alpha * m2
        delta = m1 - 2.0 * alpha * m2 + alpha * alpha * m3
        beta = gamma / m0
        step = gamma / (delta - beta * gamma / alpha)
        return (alpha + step * (1.0 + beta), -alpha * step)

    a, b = steps(*m[0:4])

    def quadratic(v):
        return v[0] + 2.0 * (a * v[1] + b * v[2]) + a * a * v[3] + 2.0 * a * b * v[4] + b * b * v[5]

    ea, eb = steps(*[quadratic(m[4 + 6 * k : 10 + 6 * k]) for k in range(4)])

    def finish(i, carry):
        row = Row(i, OWN, False)
        j = i - 4
        press_out[j] = row.at(xu, 0) + a * row.at(z0, 0) + b * row.at(sp, 0)
        for c in range(3):
            total = row.at(xu, 1 + c)
            for p in range(3):
                total = total + weights[p] * row.at(ze, 3 * p + c)
                total = total + weights[3 + p] * row.at(se, 3 * p + c)
            motion_out[c, j] = total
        total = cd[0, j]
        for k in range(6):
            total = total + weights[k] * cd[1 + k, j]
        strain_out[j] = total
        return carry

    weights = (ea, ea * a, ea * b, eb, eb * a, eb * b)
    lax.fori_loop(4, 12, finish, 0, unroll=4)
    for copy in sent:
        copy.wait_send()


def hand_over(*refs):
    src, dst, held, (come, go) = (refs[0:3], refs[3:6], refs[6:9], refs[9:11])
    incoming = [pltpu.make_async_copy(a, h, come.at[k]) for k, (a, h) in enumerate(zip(src, held))]
    outgoing = [pltpu.make_async_copy(h, b, go.at[k]) for k, (h, b) in enumerate(zip(held, dst))]
    for copy in incoming:
        copy.start()
    for copy, onward in zip(incoming, outgoing):
        copy.wait()
        onward.start()
    for onward in outgoing:
        onward.wait()


def local_step(sizes, *args):
    nx, ny, nz, cores, xs = sizes

    def field(n):
        return pltpu.VMEM((n, 18, 32, 128), F32)

    def vmem(*shape):
        return pltpu.VMEM(shape, F32)

    def strips(n):
        g = -(-n // 4)
        return (
            vmem(n, 16, 128),
            vmem(2, g, 16, 128),
            vmem(2, n, 4, 128),
            vmem(2, 2, g, 4, 128),
            vmem(2, n, 16, 128),
            vmem(2, 2, g, 16, 128),
            vmem(2, 2, n, 4, 128),
            vmem(2, 2, 2, g, 4, 128),
        )

    moving = ((4, 1), (2, 4), (1, 4), (3, 2))
    count_a, count_b = (nx // cores * nz - 1, ny * cores - 1)
    sent = max(count_a + count_b, 1)
    dma = pltpu.SemaphoreType.DMA
    scratch = [
        *[pltpu.SMEM((ZONES,), F32) for _ in range(3)],
        vmem(8, 16, 128),
        vmem(8, 16, 128),
        vmem(3, 8, 16, 128),
        pltpu.VMEM((8, 16, 128), jnp.int32),
        pltpu.VMEM((8, 16, 128), jnp.int32),
        field(2),
        field(4),
        field(1),
        field(9),
        field(4),
        field(4),
        field(4),
        field(2),
        field(6),
        field(1),
        field(3),
        field(9),
        vmem(7, 8, 16, 128),
        *[vmem(2, n, 8, d, 128) for n, d in moving],
        *[vmem(2, n, 8 + 2 * d, d, 128) for n, d in moving],
        strips(6),
        strips(4),
        vmem(32, 128),
        vmem(3, 1, 128),
        vmem(max(count_a, 1), 1, 128),
        vmem(max(count_b, 1), 1, 128),
        dma((10,)),
        dma((68,)),
        dma((68,)),
        dma((sent,)),
        dma((sent,)),
        pltpu.SemaphoreType.REGULAR,
    ]
    far = pl.BlockSpec(memory_space=pltpu.HBM)
    near = pl.BlockSpec(memory_space=pltpu.VMEM)
    done = pl.pallas_call(
        functools.partial(kernel, sizes),
        name="biot_step",
        out_shape=(
            jax.ShapeDtypeStruct((8, 16, 128), F32),
            jax.ShapeDtypeStruct((3, 8, 16, 128), F32),
            jax.ShapeDtypeStruct((8, 16, 128), F32),
        ),
        in_specs=[far] * 10,
        out_specs=(near, near, near),
        scratch_shapes=scratch,
        compiler_params=pltpu.CompilerParams(
            collective_id=0, has_side_effects=True, vmem_limit_bytes=67043328
        ),
    )(*args)
    shapes = [(8, 16, 128), (3, 8, 16, 128), (8, 16, 128)]
    return tuple(
        pl.pallas_call(
            hand_over,
            name="hand_over",
            out_shape=tuple(jax.ShapeDtypeStruct(shape, F32) for shape in shapes),
            in_specs=[far] * 3,
            out_specs=(far, far, far),
            scratch_shapes=[*[vmem(*shape) for shape in shapes], dma((3,)), dma((3,))],
        )(*done)
    )


def solution(mesh, cores=2, xs=4):
    sizes = (mesh.shape["gx"], mesh.shape["gy"], mesh.shape["gz"], cores, xs)
    scalar = P("gx", "gy", "gz")
    vector = P(None, "gx", "gy", "gz")
    return jax.shard_map(
        functools.partial(local_step, sizes),
        mesh=mesh,
        in_specs=(scalar, scalar, scalar, vector, vector, scalar, scalar, P(), P(), P()),
        out_specs=(scalar, vector, scalar),
        check_vma=False,
    )
```
